32 devices in a mesh: row: 4 (over y, core), col: 8 (over z, x).
Axes of the slice: x: 2, y: 2, z: 4, core: 2. Of those that a mesh axis runs over, the one named last changes fastest.
Arguments:
- tokens: bfloat16 [40, 8192], P('col', 'row'), may hold values from -6 to 6
- grad_out: bfloat16 [40, 8192], P('col', 'row'), may hold values from -6 to 6
- gate_weight: bfloat16 [8192, 28672], P('row', 'col'), may hold values from -0.0625 to 0.0625
- up_weight: bfloat16 [8192, 28672], P('row', 'col'), may hold values from -0.0625 to 0.0625
- down_weight: bfloat16 [28672, 8192], P('col', 'row'), may hold values from -0.03125 to 0.03125
Outputs:
- grad_tokens: bfloat16 [40, 8192], P('col', 'row')
- grad_gate_weight: bfloat16 [8192, 28672], P('row', 'col')
- grad_up_weight: bfloat16 [8192, 28672], P('row', 'col')
- grad_down_weight: bfloat16 [28672, 8192], P('col', 'row')
The draws below stay inside these ranges and needn't reach their ends.
All inputs are finite; a program needn't handle non-finite values.
Results may differ from the reference program's by a relative error of at most 0.0049.
Values may be sent and summed in bfloat16 or wider, within the bound.
A program may use at most 192 MiB of HBM per device.

```python
import jax
import jax.numpy as jnp

D = 8192
FF = 28672
TOKENS = 40


def steps_of(stream_key, dims, shards, low, top_value):
    def one(axis_at, blocks):
        steps = jax.random.uniform(jax.random.fold_in(jax.random.fold_in(stream_key, 6), axis_at), (blocks,), jnp.float32, low / len(shards), top_value / len(shards))
        return jnp.repeat(jnp.exp(steps), dims[axis_at] // blocks).reshape((-1,) + (1,) * (len(dims) - axis_at - 1))

    factor_of = one(*shards[0])
    for cut in shards[1:]:
        factor_of = factor_of * one(*cut)
    return factor_of


def gaussian(key, shape, spread, reach, pieces=(), dtype=jnp.bfloat16):
    gain = steps_of(key, shape, pieces, -0.22, 0.18) if pieces else 1.0
    array = jax.random.normal(key, shape, jnp.float32) * spread * gain
    return jnp.minimum(jnp.maximum(array, -reach), reach).astype(dtype)


def setup_inputs(seed: int = 0) -> dict:
    seeds = jax.random.split(jax.random.key(seed), 6)
    tokens = gaussian(seeds[0], (TOKENS, D), 1.0, 6.0, ((0, 8), (1, 4)))
    grad_out = gaussian(seeds[1], (TOKENS, D), 1.0, 6.0, ((0, 8), (1, 4)))
    gate_weight = gaussian(seeds[2], (D, FF), D ** -0.5, 0.0625, ((0, 4), (1, 8)))
    up_weight = gaussian(seeds[3], (D, FF), D ** -0.5, 0.0625, ((0, 4), (1, 8)))
    down_weight = gaussian(seeds[4], (FF, D), FF ** -0.5, 0.03125, ((0, 8), (1, 4)))
    return dict(tokens=tokens, grad_out=grad_out, gate_weight=gate_weight, up_weight=up_weight, down_weight=down_weight)


def hidden_grads(gate_sum, up_sum, back_sum):
    sigmoid_gate = 1.0 / (1.0 + jnp.exp(-gate_sum))
    activated = gate_sum * sigmoid_gate
    hidden = (activated * up_sum).astype(jnp.bfloat16)
    grad_up = (back_sum * activated).astype(jnp.bfloat16)
    slope = sigmoid_gate * (1.0 + gate_sum * (1.0 - sigmoid_gate))
    grad_gate = (back_sum * up_sum * slope).astype(jnp.bfloat16)
    return hidden, grad_gate, grad_up


def reference(tokens, grad_out, gate_weight, up_weight, down_weight):
    gate_sum = jnp.dot(tokens, gate_weight, preferred_element_type=jnp.float32)
    up_sum = jnp.dot(tokens, up_weight, preferred_element_type=jnp.float32)
    back_sum = jnp.dot(grad_out, down_weight.T, preferred_element_type=jnp.float32)
    hidden, grad_gate, grad_up = hidden_grads(gate_sum, up_sum, back_sum)
    grad_down_weight = jnp.dot(hidden.T, grad_out, preferred_element_type=jnp.float32).astype(jnp.bfloat16)
    grad_gate_weight = jnp.dot(tokens.T, grad_gate, preferred_element_type=jnp.float32).astype(jnp.bfloat16)
    grad_up_weight = jnp.dot(tokens.T, grad_up, preferred_element_type=jnp.float32).astype(jnp.bfloat16)
    grad_tokens = jnp.dot(grad_gate, gate_weight.T, preferred_element_type=jnp.float32)
    grad_tokens = grad_tokens + jnp.dot(grad_up, up_weight.T, preferred_element_type=jnp.float32)
    return grad_tokens.astype(jnp.bfloat16), grad_gate_weight, grad_up_weight, grad_down_weight
```

```python
import functools

import jax
import jax.numpy as jnp
from jax import lax
from jax.experimental import pallas as pl
from jax.experimental.pallas import tpu as pltpu
from jax.sharding import PartitionSpec as P

F32 = jnp.float32
BF16 = jnp.bfloat16
LAST = (((1,), (1,)), ((), ()))
MESH = pl.DeviceIdType.MESH
HALF = 256
LANES = 128
LEAD = 2
DELAY = 3
PIECES = 2
TAIL = 2


def hidden_grads(gate_sum, up_sum, back_sum):
    sigmoid_gate = 1.0 / (1.0 + jnp.exp(-gate_sum))
    activated = gate_sum * sigmoid_gate
    hidden = (activated * up_sum).astype(BF16)
    grad_up = (back_sum * activated).astype(BF16)
    slope = sigmoid_gate * (1.0 + gate_sum * (1.0 - sigmoid_gate))
    grad_gate = (back_sum * up_sum * slope).astype(BF16)
    return (hidden, grad_gate, grad_up)


def exchange_kernel(
    rows, cols, tok_in, grad_in, gate_hbm, up_hbm, down_hbm,
    tok_out, grad_out, acts_out, dtok_out,
    gate_buf, up_buf, down_buf, tok_all, grad_all, packed, slots, loose, stage, parts, pair_recv,
    chip_send, chip_recv, acts, acc, dtok_send, dtok_recv,
    load_sem, line_ssem, line_rsem, fwd_ssem, fwd_rsem, pair_ssem, pair_rsem,
    chip_ssem, chip_rsem, acts_ssem, acts_rsem, dtok_ssem, dtok_rsem, out_sem, acts_sem,
):
    row, col = lax.axis_index("row"), lax.axis_index("col")
    chips, lines = rows // 2, cols // 2
    chip, core = row // 2, row % 2
    line, side = col // 2, col % 2
    few, depth = tok_in.shape
    half = acts.shape[-1]
    span = 2 * half
    chunks = acts.shape[0]
    strips = depth // LANES
    partner = chip * 2 + (1 - core)

    def remote(src, dst, ssem, rsem, to):
        return pltpu.make_async_remote_copy(
            src_ref=src, dst_ref=dst, send_sem=ssem, recv_sem=rsem, device_id=to, device_id_type=MESH
        )

    def load(i, k):
        at = pl.ds(k * span, span)
        if i == 2:
            return pltpu.make_async_copy(down_hbm.at[at, :], down_buf.at[at, :], load_sem.at[i, k])
        src, dst = ((gate_hbm, gate_buf), (up_hbm, up_buf))[i]
        return pltpu.make_async_copy(src.at[:, at], dst.at[:, at], load_sem.at[i, k])

    order = []
    for s in range(chunks + LEAD):
        if s < chunks:
            order += [(0, s), (1, s)]
        if s >= LEAD:
            order.append((2, s - LEAD))
    early = 2 * LEAD
    for i, k in order[:early]:
        load(i, k).start()

    barrier = pltpu.get_barrier_semaphore()
    for to in [partner] + [((chip + dy) % chips) * 2 + core for dy in range(1, chips)]:
        pl.semaphore_signal(barrier, inc=1, device_id=(to, col), device_id_type=MESH)
    for s in range(1, cols):
        pl.semaphore_signal(barrier, inc=1, device_id=(row, (col + s) % cols), device_id_type=MESH)
    for a, whole in enumerate((tok_in, grad_in)):
        for j in range(strips):
            loose[a, j * few : (j + 1) * few, :] = whole[:, j * LANES : (j + 1) * LANES].astype(F32)
        mine = loose[a].astype(BF16)
        packed[a] = mine
        slots[a, col] = mine
    pl.semaphore_wait(barrier, chips + cols - 1)

    def along(a, s):
        to = ((line + s) % lines) * 2 + side
        return remote(packed.at[a], slots.at[a, col], line_ssem.at[a, s], line_rsem.at[a, s], (row, to))

    def across(a, s):
        q = ((line + lines - s) % lines) * 2 + side
        src = packed.at[a] if s == 0 else slots.at[a, q]
        return remote(src, slots.at[a, q], fwd_ssem.at[a, s], fwd_rsem.at[a, s], (row, line * 2 + 1 - side))

    for a in range(2):
        for s in range(1, lines):
            along(a, s).start()
        across(a, 0).start()
    for i, k in order[early:]:
        load(i, k).start()
    for a in range(2):
        for s in range(1, lines):
            along(a, s).wait_recv()
            across(a, s).start()

    def assemble(a, whole, out):
        for s in range(lines):
            across(a, s).wait_recv()
        for q in range(cols):
            loose[q] = slots[a, q].astype(F32)
            for j in range(strips):
                at = slice(j * LANES, (j + 1) * LANES)
                stage[q * few : (q + 1) * few, at] = loose[q, j * few : (j + 1) * few, :]
        whole[...] = stage[...].astype(BF16)
        keep = pltpu.make_async_copy(whole, out, out_sem.at[a])
        keep.start()
        return keep

    def spread(i, k, value):
        for h in range(2):
            parts[k, h, i] = value[:, h * half : (h + 1) * half]

    def pair(m, k):
        at = pl.ds(0, 2) if m == 0 else 2
        return remote(
            parts.at[k, 1 - core, at], pair_recv.at[k, at], pair_ssem.at[m, k], pair_rsem.at[m, k], (partner, col)
        )

    def chip_copy(m, k, dy):
        at = pl.ds(0, 2) if m == 0 else 2
        to = ((chip + dy) % chips) * 2 + core
        return remote(
            chip_send.at[k, at], chip_recv.at[dy - 1, k, at],
            chip_ssem.at[m, dy - 1, k], chip_rsem.at[m, dy - 1, k], (to, col),
        )

    def share(k, owner):
        return remote(acts.at[k, owner], acts.at[k, owner], acts_ssem.at[k], acts_rsem.at[k], (partner, col))

    def forward_gu(k):
        at = slice(k * span, (k + 1) * span)
        spread(0, k, jnp.dot(tok_all[...], gate_buf[:, at], preferred_element_type=F32))
        spread(1, k, jnp.dot(tok_all[...], up_buf[:, at], preferred_element_type=F32))

    def forward_back(k):
        at = slice(k * span, (k + 1) * span)
        spread(2, k, lax.dot_general(down_buf[at, :], grad_all[...], LAST, preferred_element_type=F32).T)

    def chip_sum(m, k):
        for i in (0, 1) if m == 0 else (2,):
            total = parts[k, core, i] + pair_recv[k, i]
            parts[k, core, i] = total
            chip_send[k, i] = total.astype(BF16)

    def activate(k):
        sums = []
        for i in range(3):
            total = parts[k, core, i]
            for dy in range(1, chips):
                total += chip_recv[dy - 1, k, i].astype(F32)
            sums.append(total)
        for i, value in enumerate(hidden_grads(*sums)):
            acts[k, core, i] = value

    piece = depth // PIECES
    patch = strips // PIECES

    def contribution(k, at):
        value = None
        for h in range(2):
            cut = slice(k * span + h * half, k * span + (h + 1) * half)
            for i, buf in ((1, gate_buf), (2, up_buf)):
                term = lax.dot_general(buf[at, cut], acts[k, h, i], LAST, preferred_element_type=F32)
                value = term if value is None else value + term
        return value

    def scatter(b, s):
        to = (col + s) % cols
        return remote(dtok_send.at[b, to], dtok_recv.at[b, s], dtok_ssem.at[b, s], dtok_rsem.at[b, s], (row, to))

    def keep_acts(k):
        return pltpu.make_async_copy(acts.at[k], acts_out.at[k], acts_sem.at[k])

    def back_project(k):
        for b in range(2 * PIECES):
            at = slice(b * piece // 2, (b + 1) * piece // 2)
            value = contribution(k, at)
            acc[at, :] = value if k == 0 else acc[at, :] + value

    def finish(ks):
        for b in range(PIECES):
            for c in range(2):
                at = slice(b * piece + c * piece // 2, b * piece + (c + 1) * piece // 2)
                value = acc[at, :]
                for k in ks:
                    value += contribution(k, at)
                stage[:, at] = value.T
            for q in range(cols):
                for j in range(patch):
                    at = slice(b * piece + j * LANES, b * piece + (j + 1) * LANES)
                    loose[q, j * few : (j + 1) * few, :] = stage[q * few : (q + 1) * few, at]
                dtok_send[b, q] = loose[q, : patch * few, :].astype(BF16)
            for s in range(1, cols):
                scatter(b, s).start()

    keeps = [assemble(0, tok_all, tok_out)]
    last = chunks + LEAD - 1
    for s in range(chunks + LEAD + DELAY + 2):
        if s <= last:
            if s < chunks:
                load(0, s).wait()
                load(1, s).wait()
            if s == LEAD:
                keeps.append(assemble(1, grad_all, grad_out))
            if s >= LEAD:
                load(2, s - LEAD).wait()
            if s < chunks:
                forward_gu(s)
            if s >= LEAD:
                forward_back(s - LEAD)
            if s < chunks:
                pair(0, s).start()
            if s >= LEAD:
                pair(1, s - LEAD).start()
        sums = [(m, k) for m, k in ((0, s - 1), (1, s - 1 - LEAD)) if 0 <= k < chunks]
        for m, k in sums:
            pair(m, k).wait_recv()
        k = s - LEAD - 1 - DELAY
        if 0 <= k < chunks:
            for m in range(2):
                for dy in range(1, chips):
                    chip_copy(m, k, dy).wait_recv()
        for m, j in sums:
            chip_sum(m, j)
        for m, j in sums:
            for dy in range(1, chips):
                chip_copy(m, j, dy).start()
        if 0 <= k < chunks:
            activate(k)
            share(k, core).start()
        k -= 1
        if 0 <= k < chunks:
            share(k, 1 - core).wait_recv()
            keep_acts(k).start()
            if k < chunks - TAIL:
                back_project(k)
    finish(range(chunks - TAIL, chunks))

    for b in range(PIECES):
        result = dtok_send[b, col].astype(F32)
        for s in range(1, cols):
            scatter(b, s).wait_recv()
            result += dtok_recv[b, s].astype(F32)
        loose[b, : patch * few, :] = result
        for j in range(patch):
            at = slice(b * piece + j * LANES, b * piece + (j + 1) * LANES)
            stage[:few, at] = loose[b, j * few : (j + 1) * few, :]
    dtok_out[...] = stage[:few, :].astype(BF16)

    for copy in keeps:
        copy.wait()
    for a in range(2):
        for s in range(1, lines):
            along(a, s).wait_send()
        for s in range(lines):
            across(a, s).wait_send()
    for k in range(chunks):
        keep_acts(k).wait()
        share(k, core).wait_send()
        for m in range(2):
            pair(m, k).wait_send()
            for dy in range(1, chips):
                chip_copy(m, k, dy).wait_send()
    for b in range(PIECES):
        for s in range(1, cols):
            scatter(b, s).wait_send()


def exchange(rows, cols, tokens, grad_out, gate_weight, up_weight, down_weight):
    few, depth = tokens.shape
    hidden = gate_weight.shape[1]
    many = few * cols
    chips, lines = rows // 2, cols // 2
    chunks = hidden // (2 * HALF)
    bundle = few * depth // LANES
    dma = pltpu.SemaphoreType.DMA
    any_spec = pl.BlockSpec(memory_space=pl.ANY)
    vmem_spec = pl.BlockSpec(memory_space=pltpu.VMEM)
    shape = jax.ShapeDtypeStruct
    return pl.pallas_call(
        functools.partial(exchange_kernel, rows, cols),
        out_shape=(
            shape((many, depth), BF16),
            shape((many, depth), BF16),
            shape((chunks, 2, 3, many, HALF), BF16),
            shape((few, depth), BF16),
        ),
        in_specs=[vmem_spec, vmem_spec, any_spec, any_spec, any_spec],
        out_specs=(any_spec, any_spec, any_spec, vmem_spec),
        scratch_shapes=[
            pltpu.VMEM((depth, hidden), BF16),
            pltpu.VMEM((depth, hidden), BF16),
            pltpu.VMEM((hidden, depth), BF16),
            pltpu.VMEM((many, depth), BF16),
            pltpu.VMEM((many, depth), BF16),
            pltpu.VMEM((2, bundle, LANES), BF16),
            pltpu.VMEM((2, cols, bundle, LANES), BF16),
            pltpu.VMEM((cols, bundle, LANES), F32),
            pltpu.VMEM((many, depth), F32),
            pltpu.VMEM((chunks, 2, 3, many, HALF), F32),
            pltpu.VMEM((chunks, 3, many, HALF), F32),
            pltpu.VMEM((chunks, 3, many, HALF), BF16),
            pltpu.VMEM((chips - 1, chunks, 3, many, HALF), BF16),
            pltpu.VMEM((chunks, 2, 3, many, HALF), BF16),
            pltpu.VMEM((depth, many), F32),
            pltpu.VMEM((PIECES, cols, bundle // PIECES, LANES), BF16),
            pltpu.VMEM((PIECES, cols, bundle // PIECES, LANES), BF16),
            dma((3, chunks)),
            dma((2, lines)),
            dma((2, lines)),
            dma((2, lines)),
            dma((2, lines)),
            dma((2, chunks)),
            dma((2, chunks)),
            dma((2, chips - 1, chunks)),
            dma((2, chips - 1, chunks)),
            dma((chunks,)),
            dma((chunks,)),
            dma((PIECES, cols)),
            dma((PIECES, cols)),
            dma((2,)),
            dma((chunks,)),
        ],
        compiler_params=pltpu.CompilerParams(
            collective_id=0, has_side_effects=True, vmem_limit_bytes=62 * 1024 * 1024
        ),
        name="exchange",
    )(tokens, grad_out, gate_weight, up_weight, down_weight)


def outer_kernel(
    steps, tok_hbm, grad_hbm, acts_hbm, dtok, dtok_out, gate_hbm, up_hbm, down_hbm,
    tok, grad, acts, tok_t, hidden_t, gate_buf, up_buf, down_buf, in_sem, sem,
):
    chunks, _, _, _, half = acts.shape
    depth = tok.shape[1]
    hidden = chunks * 2 * half
    part, strip = depth // steps, hidden // steps

    ins = [
        pltpu.make_async_copy(src, dst, in_sem.at[n])
        for n, (src, dst) in enumerate(((tok_hbm, tok), (acts_hbm, acts), (grad_hbm, grad)))
    ]
    for copy in ins:
        copy.start()

    def copies(slot, t):
        over = pl.ds(pl.multiple_of(t * part, part), part)
        down = pl.ds(pl.multiple_of(t * strip, 16), strip)
        return (
            pltpu.make_async_copy(gate_buf.at[slot], gate_hbm.at[over, :], sem.at[0, slot]),
            pltpu.make_async_copy(up_buf.at[slot], up_hbm.at[over, :], sem.at[1, slot]),
            pltpu.make_async_copy(down_buf.at[slot], down_hbm.at[down, :], sem.at[2, slot]),
        )

    dtok_out[...] = dtok[...]
    ins[0].wait()
    tok_t[...] = tok[...].astype(F32).T.astype(BF16)
    ins[1].wait()
    ins[2].wait()

    @pl.loop(0, steps)
    def _(t):
        slot = t % 2
        over = pl.ds(pl.multiple_of(t * part, part), part)
        down = pl.ds(pl.multiple_of(t * strip, 16), strip)
        outs = copies(slot, t)

        @pl.when(t >= 2)
        def _():
            for copy in outs:
                copy.wait()

        for n, (buf, i) in enumerate(((gate_buf, 1), (up_buf, 2))):
            for k in range(chunks):
                for h in range(2):
                    at = slice((2 * k + h) * half, (2 * k + h + 1) * half)
                    buf[slot, :, at] = jnp.dot(
                        tok_t[over, :], acts[k, h, i], preferred_element_type=F32
                    ).astype(BF16)
            outs[n].start()

        @pl.when(t == 0)
        def _():
            for k in range(chunks):
                for h in range(2):
                    at = slice((2 * k + h) * half, (2 * k + h + 1) * half)
                    hidden_t[at, :] = acts[k, h, 0].astype(F32).T.astype(BF16)

        down_buf[slot] = jnp.dot(hidden_t[down, :], grad[...], preferred_element_type=F32).astype(BF16)
        outs[2].start()

    for slot in range(2):
        for copy in copies(slot, steps - 2 + slot):
            copy.wait()


def outer(tok, grad, acts, dtok):
    many, depth = tok.shape
    chunks, _, _, _, half = acts.shape
    hidden = chunks * 2 * half
    steps = 8
    shape = jax.ShapeDtypeStruct
    any_spec = pl.BlockSpec(memory_space=pl.ANY)
    vmem_spec = pl.BlockSpec(memory_space=pltpu.VMEM)
    return pl.pallas_call(
        functools.partial(outer_kernel, steps),
        out_shape=(
            shape(dtok.shape, BF16),
            shape((depth, hidden), BF16),
            shape((depth, hidden), BF16),
            shape((hidden, depth), BF16),
        ),
        in_specs=[any_spec, any_spec, any_spec, vmem_spec],
        out_specs=(vmem_spec, any_spec, any_spec, any_spec),
        scratch_shapes=[
            pltpu.VMEM((many, depth), BF16),
            pltpu.VMEM((many, depth), BF16),
            pltpu.VMEM(acts.shape, BF16),
            pltpu.VMEM((depth, many), BF16),
            pltpu.VMEM((hidden, many), BF16),
            pltpu.VMEM((2, depth // steps, hidden), BF16),
            pltpu.VMEM((2, depth // steps, hidden), BF16),
            pltpu.VMEM((2, hidden // steps, depth), BF16),
            pltpu.SemaphoreType.DMA((3,)),
            pltpu.SemaphoreType.DMA((3, 2)),
        ],
        compiler_params=pltpu.CompilerParams(vmem_limit_bytes=62 * 1024 * 1024),
        name="outer",
    )(tok, grad, acts, dtok)


def shards(rows, cols, tokens, grad_out, gate_weight, up_weight, down_weight):
    tok, grad, acts, grad_tokens = exchange(
        rows, cols, tokens, grad_out, gate_weight, up_weight, down_weight
    )
    return outer(tok, grad, acts, grad_tokens)


def plain_shards(tokens, grad_out, gate_weight, up_weight, down_weight):
    tok_full, grad_full = (
        lax.all_gather(tokens, "col", axis=0, tiled=True),
        lax.all_gather(grad_out, "col", axis=0, tiled=True),
    )
    hidden_width = gate_weight.shape[1]
    gate_part = jnp.dot(tok_full, gate_weight, preferred_element_type=F32)
    up_part = jnp.dot(tok_full, up_weight, preferred_element_type=F32)
    back_part = jnp.einsum("td,fd->tf", grad_full, down_weight, preferred_element_type=F32)
    sums = lax.psum(jnp.concatenate([gate_part, up_part, back_part], axis=1), "row")
    hidden, grad_gate, grad_up = hidden_grads(*jnp.split(sums, 3, axis=1))
    grad_down_weight = jnp.einsum("tf,td->fd", hidden, grad_full, preferred_element_type=F32).astype(BF16)
    grad_gate_weight = jnp.einsum("td,tf->df", tok_full, grad_gate, preferred_element_type=F32).astype(BF16)
    grad_up_weight = jnp.einsum("td,tf->df", tok_full, grad_up, preferred_element_type=F32).astype(BF16)
    total = jnp.einsum("tf,df->td", grad_gate, gate_weight, preferred_element_type=F32)
    total += jnp.einsum("tf,df->td", grad_up, up_weight, preferred_element_type=F32)
    grad_tokens = lax.psum_scatter(total, "col", scatter_dimension=0, tiled=True).astype(BF16)
    return (grad_tokens, grad_gate_weight, grad_up_weight, grad_down_weight)


def choose(rows, cols, *operands):
    depth, hidden = operands[2].shape
    if hidden % (2 * HALF) or depth % (PIECES * 2 * 128) or rows % 2 or cols % 2 or rows < 4:
        return plain_shards(*operands)
    return shards(rows, cols, *operands)


def solution(mesh):
    placed = (P("col", "row"), P("col", "row"), P("row", "col"), P("row", "col"), P("col", "row"))
    return jax.shard_map(
        functools.partial(choose, mesh.shape["row"], mesh.shape["col"]),
        mesh=mesh,
        in_specs=placed,
        out_specs=(P("col", "row"), P("row", "col"), P("row", "col"), P("col", "row")),
        check_vma=False,
    )
```

```python
import functools

import jax
import jax.numpy as jnp
from jax import lax
from jax.experimental import pallas as pl
from jax.experimental.pallas import tpu as pltpu
from jax.sharding import PartitionSpec as P

F32 = jnp.float32
BF16 = jnp.bfloat16
LAST = (((1,), (1,)), ((), ()))
MESH = pl.DeviceIdType.MESH
HALF = 256
LANES = 128
LEAD = 2
DELAY = 3
PIECES = 4
TAIL = 1


def hidden_grads(gate_sum, up_sum, back_sum):
    sigmoid_gate = 1.0 / (1.0 + jnp.exp(-gate_sum))
    activated = gate_sum * sigmoid_gate
    hidden = (activated * up_sum).astype(BF16)
    grad_up = (back_sum * activated).astype(BF16)
    slope = sigmoid_gate * (1.0 + gate_sum * (1.0 - sigmoid_gate))
    grad_gate = (back_sum * up_sum * slope).astype(BF16)
    return (hidden, grad_gate, grad_up)


def exchange_kernel(
    rows, cols, tok_hbm, grad_hbm, gate_hbm, up_hbm, down_hbm,
    tok_out, grad_out, acts_out, dtok_out,
    tok_in, grad_in, gate_buf, up_buf, down_buf, tok_all, grad_all, packed, slots, loose, stage, parts, pair_recv,
    chip_send, chip_recv, acts, acc, dtok_send, dtok_recv,
    load_sem, line_ssem, line_rsem, fwd_ssem, fwd_rsem, pair_ssem, pair_rsem,
    chip_ssem, chip_rsem, acts_ssem, acts_rsem, dtok_ssem, dtok_rsem, in_sem, out_sem, acts_sem,
):
    row, col = lax.axis_index("row"), lax.axis_index("col")
    chips, lines = rows // 2, cols // 2
    chip, core = row // 2, row % 2
    line, side = col // 2, col % 2
    few, depth = tok_in.shape
    half = acts.shape[-1]
    span = 2 * half
    chunks = acts.shape[0]
    strips = depth // LANES
    partner = chip * 2 + (1 - core)

    def remote(src, dst, ssem, rsem, to):
        return pltpu.make_async_remote_copy(
            src_ref=src, dst_ref=dst, send_sem=ssem, recv_sem=rsem, device_id=to, device_id_type=MESH
        )

    def load(i, k):
        at = pl.ds(k * span, span)
        if i == 2:
            return pltpu.make_async_copy(down_hbm.at[at, :], down_buf.at[at, :], load_sem.at[i, k])
        src, dst = ((gate_hbm, gate_buf), (up_hbm, up_buf))[i]
        return pltpu.make_async_copy(src.at[:, at], dst.at[:, at], load_sem.at[i, k])

    fetches = [
        pltpu.make_async_copy(tok_hbm, tok_in, in_sem.at[0]),
        pltpu.make_async_copy(grad_hbm, grad_in, in_sem.at[1]),
    ]
    for copy in fetches:
        copy.start()

    order = []
    for s in range(chunks + LEAD):
        if s < chunks:
            order += [(0, s), (1, s)]
        if s >= LEAD:
            order.append((2, s - LEAD))
    barrier = pltpu.get_barrier_semaphore()
    for to in [partner] + [((chip + dy) % chips) * 2 + core for dy in range(1, chips)]:
        pl.semaphore_signal(barrier, inc=1, device_id=(to, col), device_id_type=MESH)
    for s in range(1, cols):
        pl.semaphore_signal(barrier, inc=1, device_id=(row, (col + s) % cols), device_id_type=MESH)
    early = len(order) // 2
    for i, k in order[:early]:
        load(i, k).start()
    for a, whole in enumerate((tok_in, grad_in)):
        fetches[a].wait()
        for j in range(strips):
            loose[a, j * few : (j + 1) * few, :] = whole[:, j * LANES : (j + 1) * LANES].astype(F32)
        mine = loose[a].astype(BF16)
        packed[a] = mine
        slots[a, col] = mine
    pl.semaphore_wait(barrier, chips + cols - 1)

    def mate(s):
        if lines != 4:
            return (line + s) % lines, (line + lines - s) % lines
        to = (line + 1 - 2 * (line % 2), (line + 2) % 4, 3 - line)[s - 1]
        return to, to

    def along(a, s):
        to = mate(s)[0] * 2 + side
        return remote(packed.at[a], slots.at[a, col], line_ssem.at[a, s], line_rsem.at[a, s], (row, to))

    def across(a, s):
        q = col if s == 0 else mate(s)[1] * 2 + side
        src = packed.at[a] if s == 0 else slots.at[a, q]
        return remote(src, slots.at[a, q], fwd_ssem.at[a, s], fwd_rsem.at[a, s], (row, line * 2 + 1 - side))

    for a in range(2):
        for s in range(lines - 1, 0, -1):
            along(a, s).start()
        across(a, 0).start()
    for i, k in order[early:]:
        load(i, k).start()
    for a in range(2):
        for s in range(1, lines):
            along(a, s).wait_recv()
            across(a, s).start()

    def assemble(a, whole, out):
        for s in range(lines):
            across(a, s).wait_recv()
        for q in range(cols):
            loose[q] = slots[a, q].astype(F32)
            for j in range(strips):
                at = slice(j * LANES, (j + 1) * LANES)
                stage[q * few : (q + 1) * few, at] = loose[q, j * few : (j + 1) * few, :]
        whole[...] = stage[...].astype(BF16)
        keep = pltpu.make_async_copy(whole, out, out_sem.at[a])
        keep.start()
        return keep

    def spread(i, k, value):
        for h in range(2):
            parts[k, h, i] = value[:, h * half : (h + 1) * half]

    def pair(m, k):
        at = pl.ds(0, 2) if m == 0 else 2
        return remote(
            parts.at[k, 1 - core, at], pair_recv.at[k, at], pair_ssem.at[m, k], pair_rsem.at[m, k], (partner, col)
        )

    def chip_copy(m, k, dy):
        at = pl.ds(0, 2) if m == 0 else 2
        to = ((chip + dy) % chips) * 2 + core
        return remote(
            chip_send.at[k, at], chip_recv.at[dy - 1, k, at],
            chip_ssem.at[m, dy - 1, k], chip_rsem.at[m, dy - 1, k], (to, col),
        )

    def share(k, owner):
        return remote(acts.at[k, owner], acts.at[k, owner], acts_ssem.at[k], acts_rsem.at[k], (partner, col))

    def forward_gu(k):
        at = slice(k * span, (k + 1) * span)
        spread(0, k, jnp.dot(tok_all[...], gate_buf[:, at], preferred_element_type=F32))
        spread(1, k, jnp.dot(tok_all[...], up_buf[:, at], preferred_element_type=F32))

    def forward_back(k):
        at = slice(k * span, (k + 1) * span)
        spread(2, k, lax.dot_general(down_buf[at, :], grad_all[...], LAST, preferred_element_type=F32).T)

    def forward_both(k, j):
        for h in range(2):
            at = slice(k * span + h * half, k * span + (h + 1) * half)
            down = slice(j * span + h * half, j * span + (h + 1) * half)
            gate_part = back_part = None
            for d in range(0, depth, half):
                cut = slice(d, d + half)
                back_term = lax.dot_general(
                    down_buf[down, cut], grad_all[:, cut], LAST, preferred_element_type=F32
                )
                gate_term = jnp.dot(tok_all[:, cut], gate_buf[cut, at], preferred_element_type=F32)
                gate_part = gate_term if d == 0 else gate_part + gate_term
                back_part = back_term if d == 0 else back_part + back_term
            parts[k, h, 0] = gate_part
            parts[j, h, 2] = back_part.T
        at = slice(k * span, (k + 1) * span)
        spread(1, k, jnp.dot(tok_all[...], up_buf[:, at], preferred_element_type=F32))

    def chip_sum(m, k):
        for i in (0, 1) if m == 0 else (2,):
            total = parts[k, core, i] + pair_recv[k, i]
            parts[k, core, i] = total
            chip_send[k, i] = total.astype(BF16)

    def activate(k):
        sums = []
        for i in range(3):
            total = parts[k, core, i]
            for dy in range(1, chips):
                total += chip_recv[dy - 1, k, i].astype(F32)
            sums.append(total)
        for i, value in enumerate(hidden_grads(*sums)):
            acts[k, core, i] = value

    piece = depth // PIECES
    patch = strips // PIECES

    def contribution(k, at):
        value = None
        for h in range(2):
            cut = slice(k * span + h * half, k * span + (h + 1) * half)
            for i, buf in ((1, gate_buf), (2, up_buf)):
                term = lax.dot_general(buf[at, cut], acts[k, h, i], LAST, preferred_element_type=F32)
                value = term if value is None else value + term
        return value

    def scatter(b, s):
        to = (col + s) % cols
        return remote(dtok_send.at[b, to], dtok_recv.at[b, s], dtok_ssem.at[b, s], dtok_rsem.at[b, s], (row, to))

    def keep_acts(k):
        return pltpu.make_async_copy(acts.at[k], acts_out.at[k], acts_sem.at[k])

    def back_project(k):
        for b in range(2 * PIECES):
            at = slice(b * piece // 2, (b + 1) * piece // 2)
            value = contribution(k, at)
            acc[at, :] = value if k == 0 else acc[at, :] + value

    def finish(ks):
        for b in range(PIECES):
            for c in range(2):
                at = slice(b * piece + c * piece // 2, b * piece + (c + 1) * piece // 2)
                value = acc[at, :]
                for k in ks:
                    value += contribution(k, at)
                stage[:, at] = value.T
            for q in range(cols):
                for j in range(patch):
                    at = slice(b * piece + j * LANES, b * piece + (j + 1) * LANES)
                    loose[q, j * few : (j + 1) * few, :] = stage[q * few : (q + 1) * few, at]
                dtok_send[b, q] = loose[q, : patch * few, :].astype(BF16)
            for s in range(1, cols):
                scatter(b, s).start()

    keeps = [assemble(0, tok_all, tok_out)]
    last = chunks + LEAD - 1
    for s in range(chunks + LEAD + DELAY + 2):
        if s <= last:
            if s < chunks:
                load(0, s).wait()
                load(1, s).wait()
            if s == LEAD:
                keeps.append(assemble(1, grad_all, grad_out))
            if s >= LEAD:
                load(2, s - LEAD).wait()
            if LEAD <= s < chunks:
                forward_both(s, s - LEAD)
            elif s < chunks:
                forward_gu(s)
            else:
                forward_back(s - LEAD)
            if s < chunks:
                pair(0, s).start()
            if s >= LEAD:
                pair(1, s - LEAD).start()
        sums = [(m, k) for m, k in ((0, s - 1), (1, s - 1 - LEAD)) if 0 <= k < chunks]
        for m, k in sums:
            pair(m, k).wait_recv()
        for m, j in sums:
            chip_sum(m, j)
        for m, j in sums:
            for dy in range(1, chips):
                chip_copy(m, j, dy).start()
        k = s - LEAD - 1 - DELAY
        if 0 <= k < chunks:
            for m in range(2):
                for dy in range(1, chips):
                    chip_copy(m, k, dy).wait_recv()
            activate(k)
            share(k, core).start()
        k -= 1
        if 0 <= k < chunks:
            share(k, 1 - core).wait_recv()
            keep_acts(k).start()
            if k < chunks - TAIL:
                back_project(k)
    finish(range(chunks - TAIL, chunks))

    for b in range(PIECES):
        result = dtok_send[b, col].astype(F32)
        for s in range(1, cols):
            scatter(b, s).wait_recv()
            result += dtok_recv[b, s].astype(F32)
        loose[b, : patch * few, :] = result
        for j in range(patch):
            at = slice(b * piece + j * LANES, b * piece + (j + 1) * LANES)
            stage[:few, at] = loose[b, j * few : (j + 1) * few, :]
    dtok_out[...] = stage[:few, :].astype(BF16)

    for copy in keeps:
        copy.wait()
    for a in range(2):
        for s in range(1, lines):
            along(a, s).wait_send()
        for s in range(lines):
            across(a, s).wait_send()
    for k in range(chunks):
        keep_acts(k).wait()
        share(k, core).wait_send()
        for m in range(2):
            pair(m, k).wait_send()
            for dy in range(1, chips):
                chip_copy(m, k, dy).wait_send()
    for b in range(PIECES):
        for s in range(1, cols):
            scatter(b, s).wait_send()


def exchange(rows, cols, tokens, grad_out, gate_weight, up_weight, down_weight):
    few, depth = tokens.shape
    hidden = gate_weight.shape[1]
    many = few * cols
    chips, lines = rows // 2, cols // 2
    chunks = hidden // (2 * HALF)
    bundle = few * depth // LANES
    dma = pltpu.SemaphoreType.DMA
    any_spec = pl.BlockSpec(memory_space=pl.ANY)
    vmem_spec = pl.BlockSpec(memory_space=pltpu.VMEM)
    shape = jax.ShapeDtypeStruct
    return pl.pallas_call(
        functools.partial(exchange_kernel, rows, cols),
        out_shape=(
            shape((many, depth), BF16),
            shape((many, depth), BF16),
            shape((chunks, 2, 3, many, HALF), BF16),
            shape((few, depth), BF16),
        ),
        in_specs=[any_spec] * 5,
        out_specs=(any_spec, any_spec, any_spec, vmem_spec),
        scratch_shapes=[
            pltpu.VMEM((few, depth), BF16),
            pltpu.VMEM((few, depth), BF16),
            pltpu.VMEM((depth, hidden), BF16),
            pltpu.VMEM((depth, hidden), BF16),
            pltpu.VMEM((hidden, depth), BF16),
            pltpu.VMEM((many, depth), BF16),
            pltpu.VMEM((many, depth), BF16),
            pltpu.VMEM((2, bundle, LANES), BF16),
            pltpu.VMEM((2, cols, bundle, LANES), BF16),
            pltpu.VMEM((cols, bundle, LANES), F32),
            pltpu.VMEM((many, depth), F32),
            pltpu.VMEM((chunks, 2, 3, many, HALF), F32),
            pltpu.VMEM((chunks, 3, many, HALF), F32),
            pltpu.VMEM((chunks, 3, many, HALF), BF16),
            pltpu.VMEM((chips - 1, chunks, 3, many, HALF), BF16),
            pltpu.VMEM((chunks, 2, 3, many, HALF), BF16),
            pltpu.VMEM((depth, many), F32),
            pltpu.VMEM((PIECES, cols, bundle // PIECES, LANES), BF16),
            pltpu.VMEM((PIECES, cols, bundle // PIECES, LANES), BF16),
            dma((3, chunks)),
            dma((2, lines)),
            dma((2, lines)),
            dma((2, lines)),
            dma((2, lines)),
            dma((2, chunks)),
            dma((2, chunks)),
            dma((2, chips - 1, chunks)),
            dma((2, chips - 1, chunks)),
            dma((chunks,)),
            dma((chunks,)),
            dma((PIECES, cols)),
            dma((PIECES, cols)),
            dma((2,)),
            dma((2,)),
            dma((chunks,)),
        ],
        compiler_params=pltpu.CompilerParams(
            collective_id=0, has_side_effects=True, vmem_limit_bytes=62 * 1024 * 1024
        ),
        name="exchange",
    )(tokens, grad_out, gate_weight, up_weight, down_weight)


def outer_kernel(
    steps, tok_hbm, grad_hbm, acts_hbm, dtok_hbm, dtok_out, gate_hbm, up_hbm, down_hbm,
    tok, grad, acts, dtok, tok_t, hidden_t, gate_buf, up_buf, down_buf, in_sem, sem,
):
    chunks, _, _, _, half = acts.shape
    depth = tok.shape[1]
    hidden = chunks * 2 * half
    part, strip = depth // steps, hidden // steps

    ins = [
        pltpu.make_async_copy(src, dst, in_sem.at[n])
        for n, (src, dst) in enumerate(((tok_hbm, tok), (acts_hbm, acts), (grad_hbm, grad), (dtok_hbm, dtok)))
    ]
    for copy in ins:
        copy.start()

    def copies(slot, t):
        down = pl.ds(pl.multiple_of(t * strip, 16), strip)
        whole = pl.ds(pl.multiple_of(t * part, part), part)
        return (
            pltpu.make_async_copy(gate_buf.at[slot], gate_hbm.at[whole, :], sem.at[0, slot]),
            pltpu.make_async_copy(up_buf.at[slot], up_hbm.at[whole, :], sem.at[1, slot]),
            pltpu.make_async_copy(down_buf.at[slot], down_hbm.at[down, :], sem.at[2, slot]),
        )

    ins[0].wait()
    tok_t[...] = tok[...].astype(F32).T.astype(BF16)
    ins[1].wait()

    @pl.loop(0, steps)
    def _(t):
        slot = t % 2
        down = pl.ds(pl.multiple_of(t * strip, 16), strip)
        outs = copies(slot, t)

        over = pl.ds(pl.multiple_of(t * part, part), part)
        for n, (buf, i) in enumerate(((gate_buf, 1), (up_buf, 2))):
            pl.when(t >= 2)(outs[n].wait)
            for k in range(chunks):
                for h in range(2):
                    at = slice((2 * k + h) * half, (2 * k + h + 1) * half)
                    buf[slot, :, at] = jnp.dot(
                        tok_t[over, :], acts[k, h, i], preferred_element_type=F32
                    ).astype(BF16)
            outs[n].start()

        @pl.when(t == 0)
        def _():
            for k in range(chunks):
                for h in range(2):
                    at = slice((2 * k + h) * half, (2 * k + h + 1) * half)
                    hidden_t[at, :] = acts[k, h, 0].astype(F32).T.astype(BF16)
            ins[2].wait()
            ins[3].wait()
            pltpu.make_async_copy(dtok, dtok_out, in_sem.at[4]).start()

        pl.when(t >= 2)(outs[2].wait)
        down_buf[slot] = jnp.dot(hidden_t[down, :], grad[...], preferred_element_type=F32).astype(BF16)
        outs[2].start()

    for slot in range(2):
        for copy in copies(slot, steps - 2 + slot):
            copy.wait()
    pltpu.make_async_copy(dtok, dtok_out, in_sem.at[4]).wait()


def outer(tok, grad, acts, dtok):
    many, depth = tok.shape
    chunks, _, _, _, half = acts.shape
    hidden = chunks * 2 * half
    steps = 4
    shape = jax.ShapeDtypeStruct
    any_spec = pl.BlockSpec(memory_space=pl.ANY)
    return pl.pallas_call(
        functools.partial(outer_kernel, steps),
        out_shape=(
            shape(dtok.shape, BF16),
            shape((depth, hidden), BF16),
            shape((depth, hidden), BF16),
            shape((hidden, depth), BF16),
        ),
        in_specs=[any_spec] * 4,
        out_specs=(any_spec,) * 4,
        scratch_shapes=[
            pltpu.VMEM((many, depth), BF16),
            pltpu.VMEM((many, depth), BF16),
            pltpu.VMEM(acts.shape, BF16),
            pltpu.VMEM(dtok.shape, BF16),
            pltpu.VMEM((depth, many), BF16),
            pltpu.VMEM((hidden, many), BF16),
            pltpu.VMEM((2, depth // steps, hidden), BF16),
            pltpu.VMEM((2, depth // steps, hidden), BF16),
            pltpu.VMEM((2, hidden // steps, depth), BF16),
            pltpu.SemaphoreType.DMA((5,)),
            pltpu.SemaphoreType.DMA((3, 2)),
        ],
        compiler_params=pltpu.CompilerParams(vmem_limit_bytes=62 * 1024 * 1024),
        name="outer",
    )(tok, grad, acts, dtok)


def shards(rows, cols, tokens, grad_out, gate_weight, up_weight, down_weight):
    tok, grad, acts, grad_tokens = exchange(
        rows, cols, tokens, grad_out, gate_weight, up_weight, down_weight
    )
    return outer(tok, grad, acts, grad_tokens)


def plain_shards(tokens, grad_out, gate_weight, up_weight, down_weight):
    tok_full, grad_full = (
        lax.all_gather(tokens, "col", axis=0, tiled=True),
        lax.all_gather(grad_out, "col", axis=0, tiled=True),
    )
    hidden_width = gate_weight.shape[1]
    gate_part = jnp.dot(tok_full, gate_weight, preferred_element_type=F32)
    up_part = jnp.dot(tok_full, up_weight, preferred_element_type=F32)
    back_part = jnp.einsum("td,fd->tf", grad_full, down_weight, preferred_element_type=F32)
    sums = lax.psum(jnp.concatenate([gate_part, up_part, back_part], axis=1), "row")
    hidden, grad_gate, grad_up = hidden_grads(*jnp.split(sums, 3, axis=1))
    grad_down_weight = jnp.einsum("tf,td->fd", hidden, grad_full, preferred_element_type=F32).astype(BF16)
    grad_gate_weight = jnp.einsum("td,tf->df", tok_full, grad_gate, preferred_element_type=F32).astype(BF16)
    grad_up_weight = jnp.einsum("td,tf->df", tok_full, grad_up, preferred_element_type=F32).astype(BF16)
    total = jnp.einsum("tf,df->td", grad_gate, gate_weight, preferred_element_type=F32)
    total += jnp.einsum("tf,df->td", grad_up, up_weight, preferred_element_type=F32)
    grad_tokens = lax.psum_scatter(total, "col", scatter_dimension=0, tiled=True).astype(BF16)
    return (grad_tokens, grad_gate_weight, grad_up_weight, grad_down_weight)


def choose(rows, cols, *operands):
    depth, hidden = operands[2].shape
    if hidden % (2 * HALF) or depth % (PIECES * 4 * 128) or rows % 2 or cols % 2 or rows < 4:
        return plain_shards(*operands)
    return shards(rows, cols, *operands)


def solution(mesh):
    placed = (P("col", "row"), P("col", "row"), P("row", "col"), P("row", "col"), P("col", "row"))
    return jax.shard_map(
        functools.partial(choose, mesh.shape["row"], mesh.shape["col"]),
        mesh=mesh,
        in_specs=placed,
        out_specs=(P("col", "row"), P("row", "col"), P("row", "col"), P("col", "row")),
        check_vma=False,
    )
```
